32 devices in a mesh: ckpt: 2 (over y), key: 4 (over x, core), qry: 4 (over z).
Axes of the slice: x: 2, y: 2, z: 4, core: 2. Of those that a mesh axis runs over, the one named last changes fastest.
Arguments:
- queries: bfloat16 [1024, 4096], P(('ckpt', 'qry'), 'key'), parts along dimension 0, may hold values from -8 to 8
- keys: bfloat16 [8192, 1024], P(('ckpt', 'key')), parts along dimension 0, may hold values from -8 to 8
- values: bfloat16 [8192, 1024], P(('ckpt', 'key')), parts along dimension 0, may hold values from -6 to 6
- out_grad: bfloat16 [1024, 4096], P(('ckpt', 'qry'), 'key'), parts along dimension 0, may hold values from -6 to 6
Outputs:
- attn_out: bfloat16 [1024, 4096], P(('ckpt', 'qry'), 'key'), parts along dimension 0
- query_out: bfloat16 [1024, 4096], P(('ckpt', 'qry'), 'key'), parts along dimension 0
- key_out: bfloat16 [8192, 1024], P(('ckpt', 'key'), 'qry'), parts along dimension 0
- value_out: bfloat16 [8192, 1024], P(('ckpt', 'key'), 'qry'), parts along dimension 0
The draws below stay inside these ranges and needn't reach their ends.
There are 2 independent parts, one for each index of `ckpt`. The reference program is written for one: setup_inputs(seed, part) draws one part's arguments, and reference() takes and returns one part's arrays. A program takes and returns all parts, laid end to end along the dimension named above; each array names one. Nothing has to cross between parts.
All inputs are finite; a program needn't handle non-finite values.
Results may differ from the reference program's by a relative error of at most 0.03.
Values may be sent and summed in bfloat16 or wider, within the bound.
No kernel may reach another device: no remote copies, remote signals or barrier semaphores. Data moves between devices by JAX's collectives and lax.ppermute only.
A program may use at most 64 MiB of HBM per device.

```python
import math
import jax
import jax.numpy as jnp
from jax import lax

HQ = 32
KVH = 8
HD = 128
Q_DEV = 128
KEY_DEV = 1024
QROWS = 512
KROWS = 4096


def draw_queries(key, part):
    sample = jax.random.normal(jax.random.fold_in(key, 11), (QROWS, HQ * HD), jnp.float32)
    sample = jnp.clip(sample, -8.0, 8.0)
    return sample.astype(jnp.bfloat16)


def draw_keys(key, part):
    sample = jax.random.normal(jax.random.fold_in(key, 21), (KROWS, KVH * HD), jnp.float32)
    sample = jnp.clip(sample, -8.0, 8.0)
    return sample.astype(jnp.bfloat16)


def block_scale(own_key, shape, cuts, least, top_value):
    def one(position, shards_of):
        heights = jax.random.uniform(jax.random.fold_in(jax.random.fold_in(own_key, 6), position), (shards_of,), jnp.float32, least / len(cuts), top_value / len(cuts))
        return jnp.repeat(jnp.exp(heights), shape[position] // shards_of).reshape((-1,) + (1,) * (len(shape) - position - 1))

    level = one(*cuts[0])
    for cut in cuts[1:]:
        level = level * one(*cut)
    return level


def gaussian(own_key, extent, deviation, reach, cuts=(), dtype=jnp.bfloat16):
    result = jax.random.normal(own_key, extent, jnp.float32) * deviation
    if len(cuts) > 0:
        result = block_scale(own_key, extent, cuts, -0.22, 0.18) * result
    return jnp.clip(result, min=-reach, max=reach).astype(dtype)


def setup_inputs(seed: int = 0, part: int = 0) -> dict:
    seeds = jax.random.split(jax.random.key(seed), 5)
    own_keys = jax.random.split(jax.random.fold_in(seeds[4], part), 5)
    return {
        "queries": draw_queries(jax.random.fold_in(jax.random.fold_in(seeds[4], part), 71), part),
        "keys": draw_keys(jax.random.fold_in(jax.random.fold_in(seeds[4], part), 71), part),
        "values": gaussian(own_keys[2], (KROWS, KVH * HD), 1.0, 6.0, ((0, 4),)),
        "out_grad": gaussian(own_keys[3], (QROWS, HQ * HD), 1.0, 6.0, ((0, 4), (1, 4))),
    }


PRECISION_HIGH = lax.Precision.HIGHEST

def rounded_values(value):
    return lax.optimization_barrier(value.astype(jnp.bfloat16)).astype(jnp.float32)

def reference(queries, keys, values, out_grad):
    per_group = HQ // KVH
    factor = 1.0 / math.sqrt(HD)
    query_count = queries.shape[0]
    key_count = keys.shape[0]
    block_count = query_count // Q_DEV
    key_blocks = key_count // KEY_DEV
    query_heads = queries.reshape(block_count, Q_DEV, KVH, per_group, HD).transpose(2, 0, 3, 1, 4)
    grad_heads = out_grad.reshape(block_count, Q_DEV, KVH, per_group, HD).transpose(2, 0, 3, 1, 4)
    key_heads = keys.reshape(key_count, KVH, HD).transpose(1, 0, 2)
    value_heads = values.reshape(key_count, KVH, HD).transpose(1, 0, 2)

    def per_head(inputs):
        query_group, grad_group, key_part, value_portion = inputs
        key_float = key_part.astype(jnp.float32)
        value_float = value_portion.astype(jnp.float32)
        value_division = value_float.reshape(key_blocks, KEY_DEV, HD)

        def per_block(running, pieces):
            query_float = pieces[0].astype(jnp.float32)
            grad_float = pieces[1].astype(jnp.float32)
            logits = jnp.einsum('grd,kd->grk', query_float, key_float, precision=PRECISION_HIGH) * factor
            split = logits.reshape(logits.shape[0], logits.shape[1], key_blocks, KEY_DEV)
            block_peak = lax.optimization_barrier(jnp.max(split, axis=-1))
            exponent_terms = jnp.exp(split - block_peak[..., None])
            block_total = lax.optimization_barrier(jnp.sum(exponent_terms, axis=-1))
            block_partial_sum = jnp.einsum('wpme,mey->wpmy', rounded_values(exponent_terms), value_division, precision=PRECISION_HIGH)
            peak = lax.optimization_barrier(jnp.max(block_peak, axis=-1))
            weight = jnp.exp(block_peak - peak[..., None])
            totals = lax.optimization_barrier(jnp.sum(weight * block_total, axis=-1))
            summed = lax.optimization_barrier(jnp.sum(block_partial_sum * weight[..., None], axis=2))
            attn_block = (summed / totals[..., None]).astype(jnp.bfloat16)
            row_delta = lax.optimization_barrier(jnp.sum(grad_float * attn_block.astype(jnp.float32), axis=-1))
            log_norm = peak + jnp.log(totals)
            probs = jnp.exp(logits - log_norm[..., None])
            grad_prob = jnp.einsum('grd,kd->grk', grad_float, value_float, precision=PRECISION_HIGH)
            grad_logit = rounded_values(probs * (grad_prob - row_delta[..., None]))
            query_grad = jnp.einsum('grk,kd->grd', grad_logit, key_float, precision=PRECISION_HIGH) * factor
            key_grad = jnp.einsum('grk,grd->kd', grad_logit, query_float, precision=PRECISION_HIGH) * factor
            value_grad = jnp.einsum('grk,grd->kd', rounded_values(probs), grad_float, precision=PRECISION_HIGH)
            updated = (running[0] + rounded_values(key_grad), running[1] + rounded_values(value_grad))
            return (updated, (attn_block, query_grad.astype(jnp.bfloat16)))
        empty = jnp.zeros((key_count, HD), jnp.float32)
        sums, outputs = lax.scan(per_block, (empty, empty), (query_group, grad_group))
        return (outputs[0], outputs[1], sums[0].astype(jnp.bfloat16), sums[1].astype(jnp.bfloat16))
    attn_heads, query_grads, key_grads, value_grads = lax.map(per_head, (query_heads, grad_heads, key_heads, value_heads))
    attn_out = attn_heads.transpose(1, 3, 0, 2, 4).reshape(query_count, HQ * HD)
    query_out = query_grads.transpose(1, 3, 0, 2, 4).reshape(query_count, HQ * HD)
    key_out = key_grads.transpose(1, 0, 2).reshape(key_count, KVH * HD)
    value_out = value_grads.transpose(1, 0, 2).reshape(key_count, KVH * HD)
    return (attn_out, query_out, key_out, value_out)
```

```python
import functools
import math

import jax
import jax.numpy as jnp
from jax import lax
from jax.experimental import pallas as pl
from jax.experimental.pallas import tpu as pltpu
from jax.sharding import PartitionSpec as P

HQ = 32
KVH = 8
HD = 128
GROUP = HQ // KVH
FACTOR = 1.0 / math.sqrt(HD)
SCALE2 = FACTOR * math.log2(math.e)

NT = (((1,), (1,)), ((), ()))
NN = (((1,), (0,)), ((), ()))


def dot(a, b, dims):
    return lax.dot_general(a, b, dims, preferred_element_type=jnp.float32)


def head(block, h):
    return block[:, h * HD : (h + 1) * HD]


def stack_heads(block, heads):
    return jnp.concatenate([head(block, h) for h in heads], axis=0)


def columns_of(rows):
    n, width = rows.shape
    pad = jnp.zeros((128 - n, width), jnp.float32)
    return jnp.concatenate([rows, pad], axis=0).T


def fwd_kernel(hp, chain, scal, q_ref, g_ref, k_ref, v_ref, o_ref, st_ref):
    rows = q_ref.shape[0]
    q, g = q_ref[...], g_ref[...]
    k, v = k_ref[...], v_ref[...]
    lane = lax.broadcasted_iota(jnp.int32, (rows, 128), 1)
    tile = jnp.zeros((rows, 128), jnp.float32)
    for first in range(0, hp, chain):
        heads = range(first, min(hp, first + chain))
        s = dot(stack_heads(q, heads), k, NT)
        m = jnp.max(s, axis=1, keepdims=True)
        p = jnp.exp2((s - m) * SCALE2)
        l = jnp.sum(p, axis=1, keepdims=True)
        o = dot(p.astype(jnp.bfloat16), v, NN)
        d = jnp.sum(o * stack_heads(g, heads).astype(jnp.float32), axis=1, keepdims=True)
        for n, h in enumerate(heads):
            part = slice(n * rows, (n + 1) * rows)
            o_ref[:, h * HD : (h + 1) * HD] = o[part].astype(jnp.bfloat16)
            tile = jnp.where(lane == h, m[part], tile)
            tile = jnp.where(lane == hp + h, l[part], tile)
            tile = jnp.where(lane == 2 * hp + h, d[part], tile)
    st_ref[0] = tile.T[: 4 * hp]


def fwd_call(qg, keys, values, scal, hp):
    rows = qg.shape[0]
    hps = qg.shape[1] // (2 * HD)
    ups = hps // hp
    nk = keys.shape[0]

    def kv_map(i, s):
        return (0, ((s[0] * ups + i) * hp) // GROUP)

    return pl.pallas_call(
        functools.partial(fwd_kernel, hp, 2),
        grid_spec=pltpu.PrefetchScalarGridSpec(
            num_scalar_prefetch=1,
            grid=(ups,),
            in_specs=[
                pl.BlockSpec((rows, hp * HD), lambda i, s: (0, i)),
                pl.BlockSpec((rows, hp * HD), lambda i, s: (0, ups + i)),
                pl.BlockSpec((nk, HD), kv_map),
                pl.BlockSpec((nk, HD), kv_map),
            ],
            out_specs=[
                pl.BlockSpec((rows, hp * HD), lambda i, s: (0, i)),
                pl.BlockSpec((1, 4 * hp, rows), lambda i, s: (i, 0, 0)),
            ],
        ),
        out_shape=[
            jax.ShapeDtypeStruct((rows, hps * HD), jnp.bfloat16),
            jax.ShapeDtypeStruct((ups, 4 * hp, rows), jnp.float32),
        ],
        cost_estimate=pl.CostEstimate(
            flops=8 * rows * hps * nk * HD, bytes_accessed=2 << 20, transcendentals=rows * hps * nk
        ),
        name="fwd",
    )(scal, qg, qg, keys, values)


def stats_kernel(hp, ups, st_ref, ld_ref):
    n_key = st_ref.shape[0]
    for u in range(n_key * ups):
        s, i = u // ups, u % ups
        parts = [st_ref[c, (s ^ c) * ups + i] for c in range(n_key)]
        peak = parts[0][:hp]
        for x in parts[1:]:
            peak = jnp.maximum(peak, x[:hp])
        total = jnp.zeros_like(peak)
        delta = jnp.zeros_like(peak)
        for x in parts:
            w = jnp.exp2((x[:hp] - peak) * SCALE2)
            total += w * x[hp : 2 * hp]
            delta += w * x[2 * hp : 3 * hp]
        ld_ref[u] = jnp.concatenate([peak * SCALE2 + jnp.log2(total), delta / total], axis=0)


def stats_call(gathered, hp, ups):
    n_key = gathered.shape[0]
    rows = gathered.shape[-1]
    return pl.pallas_call(
        functools.partial(stats_kernel, hp, ups),
        out_shape=jax.ShapeDtypeStruct((n_key * ups, 2 * hp, rows), jnp.float32),
        cost_estimate=pl.CostEstimate(flops=1 << 20, bytes_accessed=1 << 19, transcendentals=1 << 15),
        name="stats",
    )(gathered)


def out_kernel(hp, ups, n_key, scal, *refs):
    st_ref, ld_ref = refs[0], refs[1]
    parts, out_ref = refs[2 : 2 + n_key], refs[2 + n_key]
    for i in range(ups):
        norm = ld_ref[scal[0] * ups + i][:hp]
        weights = [
            jnp.exp2(st_ref[scal[p + 1], p * ups + i][:hp] * SCALE2 - norm) for p in range(n_key)
        ]
        cols = columns_of(jnp.concatenate(weights, axis=0))
        for h in range(hp):
            at = slice((i * hp + h) * HD, (i * hp + h + 1) * HD)
            total = None
            for p in range(n_key):
                lane = p * hp + h
                term = parts[p][:, at].astype(jnp.float32) * cols[:, lane : lane + 1]
                total = term if total is None else total + term
            out_ref[:, at] = total.astype(jnp.bfloat16)


def out_call(gathered, ld, parts, scal, hp, ups):
    n_key = len(parts)
    vmem = pl.BlockSpec(memory_space=pltpu.VMEM)
    return pl.pallas_call(
        functools.partial(out_kernel, hp, ups, n_key),
        in_specs=[pl.BlockSpec(memory_space=pltpu.SMEM)] + [vmem] * (2 + n_key),
        out_specs=vmem,
        out_shape=jax.ShapeDtypeStruct(parts[0].shape, jnp.bfloat16),
        cost_estimate=pl.CostEstimate(flops=1 << 22, bytes_accessed=2 << 20, transcendentals=1 << 12),
        name="attn_out",
    )(scal, gathered, ld, *parts)


def dq_kernel(hp, chain, scal, q_ref, g_ref, k_ref, v_ref, ld_ref, dq_ref):
    rows = q_ref.shape[0]
    q, g = q_ref[...], g_ref[...]
    k, v = k_ref[...], v_ref[...]
    cols = columns_of(ld_ref[0])
    for first in range(0, hp, chain):
        heads = range(first, min(hp, first + chain))
        norm = jnp.concatenate([cols[:, h : h + 1] for h in heads], axis=0)
        delta = jnp.concatenate([cols[:, hp + h : hp + h + 1] for h in heads], axis=0)
        s = dot(stack_heads(q, heads), k, NT)
        p = jnp.exp2(s * SCALE2 - norm)
        gp = dot(stack_heads(g, heads), v, NT)
        ds = (p * (gp - delta)).astype(jnp.bfloat16)
        dq = dot(ds, k, NN) * FACTOR
        for n, h in enumerate(heads):
            dq_ref[:, h * HD : (h + 1) * HD] = dq[n * rows : (n + 1) * rows].astype(jnp.bfloat16)


def dq_call(qg, keys, values, ld, scal, hp):
    rows = qg.shape[0]
    hps = qg.shape[1] // (2 * HD)
    ups = hps // hp
    nk = keys.shape[0]

    def kv_map(i, s):
        return (0, ((s[0] * ups + i) * hp) // GROUP)

    return pl.pallas_call(
        functools.partial(dq_kernel, hp, 2),
        grid_spec=pltpu.PrefetchScalarGridSpec(
            num_scalar_prefetch=1,
            grid=(ups,),
            in_specs=[
                pl.BlockSpec((rows, hp * HD), lambda i, s: (0, i)),
                pl.BlockSpec((rows, hp * HD), lambda i, s: (0, ups + i)),
                pl.BlockSpec((nk, HD), kv_map),
                pl.BlockSpec((nk, HD), kv_map),
                pl.BlockSpec((1, 2 * hp, rows), lambda i, s: (s[0] * ups + i, 0, 0)),
            ],
            out_specs=pl.BlockSpec((rows, hp * HD), lambda i, s: (0, i)),
        ),
        out_shape=jax.ShapeDtypeStruct((rows, hps * HD), jnp.bfloat16),
        cost_estimate=pl.CostEstimate(
            flops=12 * rows * hps * nk * HD, bytes_accessed=2 << 20, transcendentals=rows * hps * nk
        ),
        name="dq",
    )(scal, qg, qg, keys, values, ld)


def pack_kernel(n_qry, per_z, width, scal, *refs):
    n_key = len(refs) - 3
    parts, out_ref, sem = refs[:n_key], refs[n_key], refs[n_key + 1]
    tmp = refs[n_key + 2]
    hps_w = parts[0].shape[1] // 2
    half = pl.multiple_of(scal[1] * width, 128)

    def copies(z, i, p):
        at = i * width
        first = pltpu.make_async_copy(
            parts[p].at[:, pl.ds(half, width)], tmp.at[z, :, pl.ds(at, width)], sem.at[z, i, 0]
        )
        second = pltpu.make_async_copy(
            parts[p].at[:, pl.ds(hps_w + half, width)],
            tmp.at[z, :, pl.ds(per_z * width + at, width)],
            sem.at[z, i, 1],
        )
        return first, second

    for z in range(n_qry):
        for i in range(per_z):
            where = jnp.bitwise_xor(scal[0], z * per_z + i)
            for p in range(n_key):

                @pl.when(where == p)
                def _():
                    for c in copies(z, i, p):
                        c.start()

    for z in range(n_qry):
        for i in range(per_z):
            for c in copies(z, i, 0):
                c.wait()
        out_ref[z] = tmp[z]


def pack_call(parts, scal, n_qry, per_z, width):
    rows = parts[0].shape[0]
    shape = (n_qry, rows, 2 * per_z * width)
    return pl.pallas_call(
        functools.partial(pack_kernel, n_qry, per_z, width),
        in_specs=[pl.BlockSpec(memory_space=pltpu.SMEM)]
        + [pl.BlockSpec(memory_space=pl.ANY)] * len(parts),
        out_specs=pl.BlockSpec(memory_space=pltpu.VMEM),
        out_shape=jax.ShapeDtypeStruct(shape, jnp.bfloat16),
        scratch_shapes=[
            pltpu.SemaphoreType.DMA((n_qry, per_z, 2)),
            pltpu.VMEM(shape, jnp.bfloat16),
        ],
        cost_estimate=pl.CostEstimate(flops=1 << 20, bytes_accessed=2 << 20, transcendentals=0),
        name="pack",
    )(scal, *parts)


def dkv_kernel(hp, scal, q_ref, g_ref, k_ref, v_ref, ld_ref, *refs):
    dk_ref, dv_ref = refs[-2:]
    n_qry, rows = q_ref.shape[0], q_ref.shape[1]
    sub = GROUP // hp
    k, v = k_ref[...], v_ref[...]
    dk = dv = None
    for z in range(n_qry):
        q, g = q_ref[z], g_ref[z]
        heads = range(GROUP)
        qs, gs = stack_heads(q, heads), stack_heads(g, heads)
        units = [ld_ref[z, u] for u in range(sub)]
        norm = jnp.concatenate([units[h // hp][h % hp : h % hp + 1] for h in heads], axis=1)
        delta = jnp.concatenate(
            [units[h // hp][hp + h % hp : hp + h % hp + 1] for h in heads], axis=1
        )
        s = dot(k, qs, NT)
        p = jnp.exp2(s * SCALE2 - norm)
        gp = dot(v, gs, NT)
        ds = (p * (gp - delta)).astype(jnp.bfloat16)
        dv_z = dot(p.astype(jnp.bfloat16), gs, NN)
        dk_z = dot(ds, qs, NN)
        dv = dv_z if dv is None else dv + dv_z
        dk = dk_z if dk is None else dk + dk_z
    dk_ref[...] = (dk * FACTOR).astype(jnp.bfloat16)
    dv_ref[...] = dv.astype(jnp.bfloat16)


def dkv_call(qgz, keys, values, ldz, scal, hp, kvl, tile, into=None):
    n_qry, rows, width = qgz.shape
    nh = width // (2 * HD * GROUP)
    nk = keys.shape[0]
    sub = GROUP // hp
    wide = GROUP * HD
    out_map = lambda g, t, s: (t, s[1] + g)
    kv_map = lambda g, t, s: (t, s[0] + g)
    in_specs = [
        pl.BlockSpec((n_qry, rows, wide), lambda g, t, s: (0, 0, g)),
        pl.BlockSpec((n_qry, rows, wide), lambda g, t, s: (0, 0, nh + g)),
        pl.BlockSpec((tile, HD), kv_map),
        pl.BlockSpec((tile, HD), kv_map),
        pl.BlockSpec((n_qry, sub, 2 * hp, rows), lambda g, t, s: (0, s[1] + g, 0, 0)),
    ]
    args = [scal, qgz, qgz, keys, values, ldz]
    aliases = {}
    if into is not None:
        in_specs += [pl.BlockSpec(memory_space=pl.ANY)] * 2
        aliases = {len(args): 0, len(args) + 1: 1}
        args += list(into)
    shape = jax.ShapeDtypeStruct((nk, kvl * HD), jnp.bfloat16)
    return pl.pallas_call(
        functools.partial(dkv_kernel, hp),
        grid_spec=pltpu.PrefetchScalarGridSpec(
            num_scalar_prefetch=1,
            grid=(nh, nk // tile),
            in_specs=in_specs,
            out_specs=[pl.BlockSpec((tile, HD), out_map)] * 2,
        ),
        out_shape=[shape, shape],
        input_output_aliases=aliases,
        cost_estimate=pl.CostEstimate(
            flops=8 * n_qry * rows * GROUP * nh * nk * HD,
            bytes_accessed=4 << 20,
            transcendentals=n_qry * rows * GROUP * nh * nk,
        ),
        name="dkv",
    )(*args)


def per_device(queries, keys, values, out_grad):
    n_key, n_qry = lax.axis_size("key"), lax.axis_size("qry")
    me_k, me_z = lax.axis_index("key"), lax.axis_index("qry")
    rows = queries.shape[0]
    hps = HQ // n_key
    hp = min(hps, GROUP)
    ups = hps // hp
    kvl = KVH // n_qry
    per_z = n_key // n_qry
    split = 2 if (kvl % 2 == 0 and per_z == 1) else 1

    def swap(x, p):
        return lax.ppermute(x, "key", [(i, i ^ p) for i in range(n_key)])

    parts = {0: jnp.concatenate([queries, out_grad], axis=1)}
    bit = n_key // 2
    while bit:
        for p in list(parts):
            parts[p ^ bit] = swap(parts[p], bit)
        bit //= 2

    order = [p for p in (0, 1)] + [p for p in range(2, n_key)]
    slice_of = [jnp.bitwise_xor(me_k, p).astype(jnp.int32) for p in range(n_key)]
    o_part, st_part = {}, {}
    for p in order:
        o_part[p], st_part[p] = fwd_call(parts[p], keys, values, slice_of[p][None], hp)

    half = (me_k % split).astype(jnp.int32)
    packed = pack_call(
        [parts[p] for p in range(n_key)],
        jnp.stack([me_k.astype(jnp.int32), half]),
        n_qry,
        per_z,
        hps * HD // split,
    )
    mine_z = lax.all_to_all(packed, "qry", split_axis=0, concat_axis=0, tiled=True)

    o_recv = [o_part[0]] + [swap(o_part[p], p) for p in range(1, n_key)]
    stats = jnp.concatenate([st_part[p] for p in range(n_key)], axis=0)
    gathered = lax.all_gather(stats, "key", axis=0, tiled=False)
    ld = stats_call(gathered, hp, ups)

    ldz = lax.all_to_all(ld, "qry", split_axis=0, concat_axis=0, tiled=True)
    ldz = ldz.reshape(n_qry, kvl * (GROUP // hp), 2 * hp, rows)

    dq_recv = {}
    for p in reversed(order):
        dq = dq_call(parts[p], keys, values, ld, slice_of[p][None], hp)
        dq_recv[p] = swap(dq, p) if p else dq

    attn_out = out_call(gathered, ld, o_recv, jnp.stack([me_k.astype(jnp.int32)] + slice_of), hp, ups)

    tile = min(512, keys.shape[0])
    z32 = me_z.astype(jnp.int32)
    if split == 2:
        nh = kvl // 2
        first = half * nh
        second = (1 - half) * nh
        other_z = swap(mine_z, 1)
        outs = dkv_call(
            mine_z, keys, values, ldz, jnp.stack([z32 * kvl + first, first]), hp, kvl, tile
        )
        outs = dkv_call(
            other_z, keys, values, ldz, jnp.stack([z32 * kvl + second, second]), hp, kvl, tile, outs
        )
    else:
        outs = dkv_call(
            mine_z, keys, values, ldz, jnp.stack([z32 * kvl, jnp.zeros_like(z32)]), hp, kvl, tile
        )

    query_out = sum(dq_recv[p].astype(jnp.float32) for p in range(n_key)).astype(jnp.bfloat16)
    return (attn_out, query_out, outs[0], outs[1])


def solution(mesh):
    in_specs = (
        P(("ckpt", "qry"), "key"),
        P(("ckpt", "key"), None),
        P(("ckpt", "key"), None),
        P(("ckpt", "qry"), "key"),
    )
    out_specs = (
        P(("ckpt", "qry"), "key"),
        P(("ckpt", "qry"), "key"),
        P(("ckpt", "key"), "qry"),
        P(("ckpt", "key"), "qry"),
    )
    return jax.shard_map(
        per_device, mesh=mesh, in_specs=in_specs, out_specs=out_specs, check_vma=False
    )
```

```python
import functools
import math

import jax
import jax.numpy as jnp
from jax import lax
from jax.experimental import pallas as pl
from jax.experimental.pallas import tpu as pltpu
from jax.sharding import PartitionSpec as P


HQ = 32
KVH = 8
HD = 128
GROUP = HQ // KVH
FACTOR = 1.0 / math.sqrt(HD)
SCALE2 = FACTOR * math.log2(math.e)
MIB = 1 << 20

NT = (((1,), (1,)), ((), ()))
NN = (((1,), (0,)), ((), ()))
BF16 = jnp.bfloat16
F32 = jnp.float32


VMEM = pl.BlockSpec(memory_space=pltpu.VMEM)


def call(kernel, out_shape, args, flops=1 << 20, limit=20 * MIB):
    def body(*refs):
        kernel((lax.axis_index("key"), lax.axis_index("qry")), *refs)

    return pl.pallas_call(
        body,
        in_specs=[VMEM] * len(args),
        out_specs=jax.tree.map(lambda _: VMEM, out_shape),
        out_shape=out_shape,
        cost_estimate=pl.CostEstimate(flops=flops, bytes_accessed=MIB, transcendentals=0),
        compiler_params=pltpu.CompilerParams(vmem_limit_bytes=limit),
    )(*args)


def shaped(shape, dtype):
    return jax.ShapeDtypeStruct(tuple(shape), dtype)


def dot(a, b, dims):
    return lax.dot_general(a, b, dims, preferred_element_type=F32)


def stack_heads(ref, base, count):
    return jnp.concatenate([ref[:, base + h * HD : base + (h + 1) * HD] for h in range(count)], axis=0)


def columns_of(rows):
    n, width = rows.shape
    pad = jnp.zeros((128 - n, width), F32)
    return jnp.concatenate([rows, pad], axis=0).T


def rows_of(columns, height):
    rows = columns[0].shape[0]
    lane = lax.broadcasted_iota(jnp.int32, (rows, 128), 1)
    tile = jnp.zeros((rows, 128), F32)
    for i, c in enumerate(columns):
        tile = jnp.where(lane == i, c, tile)
    return tile.T[:height]


def kv_column(scal, p, i, ups, hp):
    g = ((scal[0] ^ p) * ups + i) * hp // GROUP
    return pl.ds(pl.multiple_of(g * HD, HD), HD)


def fwd_kernel(hp, ups, places, scal, *refs):
    n = len(places)
    q_refs, (k_ref, v_ref) = refs[:n], refs[n : n + 2]
    o_refs, st_ref = refs[-n - 1 : -1], refs[-1]
    rows = q_refs[0].shape[0]
    for at, p in enumerate(places):
        for i in range(ups):
            col = kv_column(scal, p, i, ups, hp)
            base = i * hp * HD
            s = dot(stack_heads(q_refs[at], base, hp), k_ref[:, col], NT)
            m = jnp.max(s, axis=1, keepdims=True)
            e = jnp.exp2((s - m) * SCALE2)
            l = jnp.sum(e, axis=1, keepdims=True)
            o = dot(e.astype(BF16), v_ref[:, col], NN).astype(BF16)
            cols = []
            for h in range(hp):
                o_refs[at][:, base + h * HD : base + (h + 1) * HD] = o[h * rows : (h + 1) * rows]
            for x in (m, l):
                cols += [x[h * rows : (h + 1) * rows] for h in range(hp)]
            st_ref[at * ups + i] = rows_of(cols, 2 * hp)


def fwd_call(places, q, keys, values, hp, ups):
    rows, wide = q[places[0]].shape
    nk = keys.shape[0]
    out = [shaped((rows, wide), BF16)] * len(places)
    out += [shaped((len(places) * ups, 2 * hp, rows), F32)]
    res = call(
        functools.partial(fwd_kernel, hp, ups, places),
        out,
        [q[p] for p in places] + [keys, values],
        flops=4 * len(places) * rows * wide * nk,
    )
    return res[:-1], res[-1]


def delta_kernel(hp, ups, n, scal, *refs):
    o_refs, g_refs, st_refs, out_ref = refs[:n], refs[n : 2 * n], refs[2 * n : -1], refs[-1]
    for p in range(n):
        for i in range(ups):
            cols = []
            for h in range(hp):
                at = slice((i * hp + h) * HD, (i * hp + h + 1) * HD)
                product = o_refs[p][:, at].astype(F32) * g_refs[p][:, at].astype(F32)
                cols.append(jnp.sum(product, axis=1, keepdims=True))
            u = p * ups + i
            out_ref[u, : 2 * hp] = st_refs[p // 2][(p % 2) * ups + i]
            out_ref[u, 2 * hp : 3 * hp] = rows_of(cols, hp)


def stats_kernel(hp, ups, n, unit_z, scal, *refs):
    st_refs, ld_ref, z_refs = refs[:n], refs[n], refs[n + 1 :]
    for p in range(n):
        for i in range(ups):
            parts = [st_refs[q][(p ^ q) * ups + i] for q in range(n)]
            peak = parts[0][:hp]
            for x in parts[1:]:
                peak = jnp.maximum(peak, x[:hp])
            total = jnp.zeros_like(peak)
            delta = jnp.zeros_like(peak)
            for x in parts:
                w = jnp.exp2((x[:hp] - peak) * SCALE2)
                total += w * x[hp : 2 * hp]
                delta += w * x[2 * hp : 3 * hp]
            both = jnp.concatenate([peak * SCALE2 + jnp.log2(total), delta / total], axis=0)
            ld_ref[(scal[0] ^ p) * ups + i] = both
    for j, ref in enumerate(z_refs):
        ref[...] = ld_ref[pl.ds((scal[1] ^ j) * unit_z, unit_z)]


def out_kernel(hp, ups, n, scal, ld_ref, *refs):
    st_refs, parts, out_ref = refs[:n], refs[n : 2 * n], refs[2 * n]
    for i in range(ups):
        norm = ld_ref[scal[0] * ups + i][:hp]
        weights = [jnp.exp2(st_refs[q][q * ups + i][:hp] * SCALE2 - norm) for q in range(n)]
        cols = columns_of(jnp.concatenate(weights, axis=0))
        for h in range(hp):
            at = slice((i * hp + h) * HD, (i * hp + h + 1) * HD)
            total = None
            for q in range(n):
                lane = q * hp + h
                term = parts[q][:, at].astype(F32) * cols[:, lane : lane + 1]
                total = term if total is None else total + term
            out_ref[:, at] = total.astype(BF16)


def dq_kernel(hp, ups, places, scal, *refs):
    n = len(places)
    q_refs, g_refs = refs[:n], refs[n : 2 * n]
    k_ref, v_ref, ld_ref = refs[2 * n : 2 * n + 3]
    dq_refs = refs[-n:]
    rows = q_refs[0].shape[0]
    for at, p in enumerate(places):
        for i in range(ups):
            col = kv_column(scal, p, i, ups, hp)
            base = i * hp * HD
            cols = columns_of(ld_ref[(scal[0] ^ p) * ups + i])
            norm = jnp.concatenate([cols[:, h : h + 1] for h in range(hp)], axis=0)
            delta = jnp.concatenate([cols[:, hp + h : hp + h + 1] for h in range(hp)], axis=0)
            k = k_ref[:, col]
            s = dot(stack_heads(q_refs[at], base, hp), k, NT)
            e = jnp.exp2(s * SCALE2 - norm)
            gp = dot(stack_heads(g_refs[at], base, hp), v_ref[:, col], NT)
            ds = (e * (gp - delta)).astype(BF16)
            dq = (dot(ds, k, NN) * FACTOR).astype(BF16)
            for h in range(hp):
                dq_refs[at][:, base + h * HD : base + (h + 1) * HD] = dq[h * rows : (h + 1) * rows]


def dq_call(places, q, g, keys, values, ld, hp, ups):
    rows, wide = q[places[0]].shape
    return call(
        functools.partial(dq_kernel, hp, ups, places),
        [shaped((rows, wide), BF16)] * len(places),
        [q[p] for p in places] + [g[p] for p in places] + [keys, values, ld],
        flops=6 * len(places) * rows * wide * keys.shape[0],
    )


def pack_kernel(split, per_z, n, n_qry, scal, *refs):
    parts, outs = refs[: 2 * n], refs[2 * n :]
    width = parts[0].shape[1] // split
    start = pl.multiple_of((scal[0] % split) * width, HD) if split > 1 else 0
    for j in range(n_qry):
        for i in range(per_z):
            place = scal[0] ^ ((scal[1] ^ j) * per_z + i)
            for p in range(n):

                @pl.when(place == p)
                def _():
                    for kind in range(2):
                        at = (kind * per_z + i) * width
                        outs[j][:, at : at + width] = parts[kind * n + p][:, pl.ds(start, width)]


def dkv_kernel(hp, kvl, nh, n_qry, which, scal, *refs):
    qg_refs, ld_refs = refs[:n_qry], refs[n_qry : 2 * n_qry]
    k_ref, v_ref = refs[2 * n_qry : 2 * n_qry + 2]
    prior, (dk_ref, dv_ref) = refs[2 * n_qry + 2 : -2], refs[-2:]
    sub = GROUP // hp
    first = 0 if which is None else ((scal[0] % 2) ^ which) * nh
    for g in range(nh):
        col = pl.ds(pl.multiple_of((scal[1] * kvl + first + g) * HD, HD), HD)
        k, v = k_ref[:, col], v_ref[:, col]
        dk = dv = None
        for qg, ld in zip(qg_refs, ld_refs):
            base = g * GROUP * HD
            qs = stack_heads(qg, base, GROUP)
            gs = stack_heads(qg, nh * GROUP * HD + base, GROUP)
            units = [ld[(first + g) * sub + u] for u in range(sub)]
            norm = jnp.concatenate([units[h // hp][h % hp : h % hp + 1] for h in range(GROUP)], axis=1)
            delta = jnp.concatenate(
                [units[h // hp][hp + h % hp : hp + h % hp + 1] for h in range(GROUP)], axis=1
            )
            s = dot(k, qs, NT)
            e = jnp.exp2(s * SCALE2 - norm)
            gp = dot(v, gs, NT)
            ds = (e * (gp - delta)).astype(BF16)
            dv_z = dot(e.astype(BF16), gs, NN)
            dk_z = dot(ds, qs, NN)
            dv = dv_z if dv is None else dv + dv_z
            dk = dk_z if dk is None else dk + dk_z
        if which == 1:
            mine = pl.ds(pl.multiple_of((first + g) * HD, HD), HD)
        else:
            mine = pl.ds(g * HD, HD)
        dk_ref[:, mine] = (dk * FACTOR).astype(BF16)
        dv_ref[:, mine] = dv.astype(BF16)
    if which == 1:
        other = pl.ds(pl.multiple_of((scal[0] % 2) * nh * HD, HD), nh * HD)
        dk_ref[:, other] = prior[0][...]
        dv_ref[:, other] = prior[1][...]


def dkv_call(qg, keys, values, ldz, hp, kvl, which=None, prior=()):
    n_qry = len(qg)
    rows, width = qg[0].shape
    nh = width // (2 * HD * GROUP)
    nk = keys.shape[0]
    out_heads = nh if which == 0 else kvl
    return call(
        functools.partial(dkv_kernel, hp, kvl, nh, n_qry, which),
        [shaped((nk, out_heads * HD), BF16)] * 2,
        list(qg) + list(ldz) + [keys, values] + list(prior),
        flops=8 * n_qry * rows * GROUP * nh * nk * HD,
        limit=24 * MIB,
    )


def sum_kernel(scal, *refs):
    total = refs[0][...].astype(F32)
    for r in refs[1:-1]:
        total += r[...].astype(F32)
    refs[-1][...] = total.astype(BF16)


def program(queries, keys, values, out_grad):
    n_key, n_qry = lax.axis_size("key"), lax.axis_size("qry")
    rows, wide = queries.shape
    hps = HQ // n_key
    hp = min(hps, GROUP)
    ups = hps // hp
    kvl = KVH // n_qry
    per_z = n_key // n_qry
    split = 2 if (kvl % 2 == 0 and per_z == 1) else 1
    unit_z = kvl * GROUP // hp

    def swap(x, p, axis="key"):
        if p == 0:
            return x
        return lax.ppermute(x, axis, [(i, i ^ p) for i in range(lax.axis_size(axis))])

    q, g = {0: queries}, {0: out_grad}
    bit = n_key // 2
    while bit:
        for p in list(q):
            q[p ^ bit] = swap(q[p], bit)
            g[p ^ bit] = swap(g[p], bit)
        bit //= 2

    o_part, st = {}, []
    for p in range(0, n_key, 2):
        o, stat = fwd_call((p, p + 1), q, keys, values, hp, ups)
        o_part[p], o_part[p + 1] = o
        st.append(stat)
    ql, gl, ol = ([x[p] for p in range(n_key)] for x in (q, g, o_part))

    packed = call(
        functools.partial(pack_kernel, split, per_z, n_key, n_qry),
        [shaped((rows, 2 * per_z * wide // split), BF16)] * n_qry,
        ql + gl,
    )
    mine_z = [swap(x, j, "qry") for j, x in enumerate(packed)]

    own = call(
        functools.partial(delta_kernel, hp, ups, n_key),
        shaped((n_key * ups, 3 * hp, rows), F32),
        ol + gl + st,
    )
    stats = [swap(own, p) for p in range(n_key)]
    o_recv = [swap(ol[p], p) for p in range(n_key)]
    ld, *ldz = call(
        functools.partial(stats_kernel, hp, ups, n_key, unit_z),
        [shaped((n_key * ups, 2 * hp, rows), F32)] + [shaped((unit_z, 2 * hp, rows), F32)] * n_qry,
        stats,
    )
    ldz = [swap(x, j, "qry") for j, x in enumerate(ldz)]

    dq_recv = [None] * n_key
    for p in reversed(range(0, n_key, 2)):
        dqs = dq_call((p, p + 1), q, g, keys, values, ld, hp, ups)
        for at, dq in enumerate(dqs):
            dq_recv[p + at] = swap(dq, p + at)

    attn_out = call(
        functools.partial(out_kernel, hp, ups, n_key),
        shaped((rows, wide), BF16),
        [ld] + stats + o_recv,
    )

    if split == 2:
        other_z = [swap(x, 1) for x in mine_z]
        prior = dkv_call(mine_z, keys, values, ldz, hp, kvl, 0)
        key_out, value_out = dkv_call(other_z, keys, values, ldz, hp, kvl, 1, prior)
    else:
        key_out, value_out = dkv_call(mine_z, keys, values, ldz, hp, kvl)

    query_out = call(sum_kernel, shaped((rows, wide), BF16), dq_recv)
    return (attn_out, query_out, key_out, value_out)


def solution(mesh):
    in_specs = (
        P(("ckpt", "qry"), "key"),
        P(("ckpt", "key"), None),
        P(("ckpt", "key"), None),
        P(("ckpt", "qry"), "key"),
    )
    out_specs = (
        P(("ckpt", "qry"), "key"),
        P(("ckpt", "qry"), "key"),
        P(("ckpt", "key"), "qry"),
        P(("ckpt", "key"), "qry"),
    )
    return jax.shard_map(
        program, mesh=mesh, in_specs=in_specs, out_specs=out_specs, check_vma=False
    )
```

```python
import functools
import math

import jax
import jax.numpy as jnp
from jax import lax
from jax.experimental import pallas as pl
from jax.experimental.pallas import tpu as pltpu
from jax.sharding import PartitionSpec as P


HQ = 32
KVH = 8
HD = 128
GROUP = HQ // KVH
FACTOR = 1.0 / math.sqrt(HD)
SCALE2 = FACTOR * math.log2(math.e)
MIB = 1 << 20
WARM_FLOPS = 1 << 33
EARLY = 2

NT = (((1,), (1,)), ((), ()))
NN = (((1,), (0,)), ((), ()))
BF16 = jnp.bfloat16
F32 = jnp.float32


VMEM = pl.BlockSpec(memory_space=pltpu.VMEM)
HBM = pl.BlockSpec(memory_space=pltpu.HBM)


def call(kernel, out_shape, args, flops=1 << 20, limit=20 * MIB, hbm=(), scratch=()):
    def body(*refs):
        kernel((lax.axis_index("key"), lax.axis_index("qry")), *refs)

    return pl.pallas_call(
        body,
        in_specs=[VMEM] * len(args),
        out_specs=[HBM if i in hbm else VMEM for i in range(len(out_shape))]
        if isinstance(out_shape, list)
        else VMEM,
        out_shape=out_shape,
        scratch_shapes=list(scratch),
        cost_estimate=pl.CostEstimate(flops=flops, bytes_accessed=MIB, transcendentals=0),
        compiler_params=pltpu.CompilerParams(vmem_limit_bytes=limit),
    )(*args)


def shaped(shape, dtype):
    return jax.ShapeDtypeStruct(tuple(shape), dtype)


def dot(a, b, dims):
    return lax.dot_general(a, b, dims, preferred_element_type=F32)


def stack_heads(ref, rows, base, count):
    parts = [ref[:rows, base + h * HD : base + (h + 1) * HD] for h in range(count)]
    return jnp.concatenate(parts, axis=0)


def columns_of(rows):
    n, width = rows.shape
    pad = jnp.zeros((128 - n, width), F32)
    return jnp.concatenate([rows, pad], axis=0).T


def rows_of(columns, height):
    rows = columns[0].shape[0]
    lane = lax.broadcasted_iota(jnp.int32, (rows, 128), 1)
    tile = jnp.zeros((rows, 128), F32)
    for i, c in enumerate(columns):
        tile = jnp.where(lane == i, c, tile)
    return tile.T[:height]


def kv_column(scal, p, i, ups, hp):
    g = ((scal[0] ^ p) * ups + i) * hp // GROUP
    return pl.ds(pl.multiple_of(g * HD, HD), HD)


def fwd_unit(hp, q, k, v, o_ref, e_ref, base, rows):
    s = dot(q, k, NT)
    m = jnp.max(s, axis=1, keepdims=True)
    e = jnp.exp2((s - m) * SCALE2)
    l = jnp.sum(e, axis=1, keepdims=True)
    e = e.astype(BF16)
    e_ref[base // HD * rows : (base // HD + hp) * rows] = e
    o = dot(e, v, NN).astype(BF16)
    cols = []
    for h in range(hp):
        o_ref[:, base + h * HD : base + (h + 1) * HD] = o[h * rows : (h + 1) * rows]
    for x in (m, l):
        cols += [x[h * rows : (h + 1) * rows] for h in range(hp)]
    return rows_of(cols, 2 * hp)


def fwd_kernel(hp, ups, places, scal, *refs):
    n = len(places)
    q_refs, (k_ref, v_ref) = refs[:n], refs[n : n + 2]
    o_refs, e_refs, st_ref = refs[-2 * n - 1 : -n - 1], refs[-n - 1 : -1], refs[-1]
    rows = q_refs[0].shape[0]
    for at, p in enumerate(places):
        for i in range(ups):
            col = kv_column(scal, p, i, ups, hp)
            base = i * hp * HD
            q = stack_heads(q_refs[at], rows, base, hp)
            st_ref[at * ups + i] = fwd_unit(
                hp, q, k_ref[:, col], v_ref[:, col], o_refs[at], e_refs[at], base, rows
            )


def fwd_shapes(n, rows, wide, nk, hp, ups):
    out = [shaped((rows, wide), BF16)] * n
    out += [shaped((rows * wide // HD, nk), BF16)] * n
    return out + [shaped((n * ups, 2 * hp, rows), F32)]


def warm_kernel(scal, out_ref):
    out_ref[...] = jnp.zeros_like(out_ref)


def warm_call():
    return call(warm_kernel, shaped((8, 128), F32), [], flops=WARM_FLOPS)


def fwd_call(places, q, keys, values, hp, ups, after=()):
    rows, wide = q[places[0]].shape
    nk = keys.shape[0]
    n = len(places)
    res = call(
        functools.partial(fwd_kernel, hp, ups, places),
        fwd_shapes(n, rows, wide, nk, hp, ups),
        [q[p] for p in places] + [keys, values] + list(after),
        flops=4 * n * rows * wide * nk,
    )
    return res[:n], res[n : 2 * n], res[-1]


def delta_kernel(hp, ups, places, whole, scal, *refs):
    n = len(places)
    o_refs, g_refs, out_ref = refs[:n], refs[n : 2 * n], refs[-1]
    st_refs = refs[2 * n : -1]
    u = 0
    if whole:
        u = whole - n * ups
        out_ref[:u] = st_refs[-1][...]
        st_refs = st_refs[:-1]
    stats = [(ref, i) for ref in st_refs for i in range(ref.shape[0])]
    for at in range(n):
        for i in range(ups):
            cols = []
            for h in range(hp):
                col = slice((i * hp + h) * HD, (i * hp + h + 1) * HD)
                product = o_refs[at][:, col].astype(F32) * g_refs[at][:, col].astype(F32)
                cols.append(jnp.sum(product, axis=1, keepdims=True))
            ref, m = stats[at * ups + i]
            out_ref[u, : 2 * hp] = ref[m]
            out_ref[u, 2 * hp : 3 * hp] = rows_of(cols, hp)
            u += 1


def split_bf16(x):
    parts = []
    for _ in range(3):
        parts.append(x.astype(BF16))
        x = x - parts[-1].astype(F32)
    return parts


def stats_kernel(hp, ups, n, unit_z, late, split, per_z, scal, *refs):
    st_refs, parts = refs[:n], refs[n : 3 * n]
    ld_ref, own_ref, early_ref = refs[3 * n : 3 * n + 3]
    outs = refs[3 * n + 3 :]
    for p in range(n):
        for i in range(ups):
            rows = [st_refs[q][(p ^ q) * ups + i] for q in range(n)]
            peak = rows[0][:hp]
            for x in rows[1:]:
                peak = jnp.maximum(peak, x[:hp])
            total = jnp.zeros_like(peak)
            delta = jnp.zeros_like(peak)
            for x in rows:
                w = jnp.exp2((x[:hp] - peak) * SCALE2)
                total += w * x[hp : 2 * hp]
                delta += w * x[2 * hp : 3 * hp]
            both = jnp.concatenate([peak * SCALE2 + jnp.log2(total), delta / total], axis=0)
            ld_ref[(scal[0] ^ p) * ups + i] = both
    own_ref[...] = ld_ref[pl.ds(scal[1] * unit_z, unit_z)]
    early_ref[...] = ld_ref[pl.ds((scal[1] ^ EARLY) * unit_z, unit_z)]
    for at, j in enumerate(late):
        pack_block(split, per_z, n, j, scal, parts, outs[at])
        block = ld_ref[pl.ds((scal[1] ^ j) * unit_z, unit_z)]
        flat = jnp.concatenate([block[u] for u in range(unit_z)], axis=0)
        height, rows = flat.shape
        for third, x in enumerate(split_bf16(flat)):
            outs[at][rows : rows + height, third * rows : (third + 1) * rows] = x


def out_kernel(hp, ups, n, scal, ld_ref, *refs):
    st_refs, parts, out_ref = refs[:n], refs[n : 2 * n], refs[2 * n]
    for i in range(ups):
        norm = ld_ref[scal[0] * ups + i][:hp]
        weights = [jnp.exp2(st_refs[q][q * ups + i][:hp] * SCALE2 - norm) for q in range(n)]
        cols = columns_of(jnp.concatenate(weights, axis=0))
        for h in range(hp):
            at = slice((i * hp + h) * HD, (i * hp + h + 1) * HD)
            total = None
            for q in range(n):
                lane = q * hp + h
                term = parts[q][:, at].astype(F32) * cols[:, lane : lane + 1]
                total = term if total is None else total + term
            out_ref[:, at] = total.astype(BF16)


def dq_kernel(hp, ups, places, scal, *refs):
    n = len(places)
    e_refs, g_refs = refs[:n], refs[n : 2 * n]
    k_ref, v_ref, ld_ref, st_ref = refs[2 * n : 2 * n + 4]
    dq_refs = refs[-n:]
    rows = g_refs[0].shape[0]
    for at, p in enumerate(places):
        for i in range(ups):
            col = kv_column(scal, p, i, ups, hp)
            base = i * hp * HD
            ld = ld_ref[(scal[0] ^ p) * ups + i]
            weight = jnp.exp2(st_ref[p * ups + i][:hp] * SCALE2 - ld[:hp]) * FACTOR
            cols = columns_of(jnp.concatenate([weight, ld[hp:]], axis=0))
            delta = jnp.concatenate([cols[:, hp + h : hp + h + 1] for h in range(hp)], axis=0)
            e = e_refs[at][base // HD * rows : (base // HD + hp) * rows]
            gp = dot(stack_heads(g_refs[at], rows, base, hp), v_ref[:, col], NT)
            ds = (e.astype(F32) * (gp - delta)).astype(BF16)
            dq = dot(ds, k_ref[:, col], NN)
            for h in range(hp):
                block = dq[h * rows : (h + 1) * rows] * cols[:, h : h + 1]
                dq_refs[at][:, base + h * HD : base + (h + 1) * HD] = block.astype(BF16)


def dq_call(places, e, g, keys, values, ld, own, hp, ups):
    rows, wide = g[places[0]].shape
    return call(
        functools.partial(dq_kernel, hp, ups, places),
        [shaped((rows, wide), BF16)] * len(places),
        [e[p] for p in places] + [g[p] for p in places] + [keys, values, ld, own],
        flops=4 * len(places) * rows * wide * keys.shape[0],
    )


def pack_block(split, per_z, n, j, scal, parts, out, other=None):
    rows, width = parts[0].shape[0], parts[0].shape[1] // split
    share = scal[0] % split if split > 1 else 0
    for i in range(per_z):
        place = scal[0] ^ ((scal[1] ^ j) * per_z + i)
        for p in range(n):

            @pl.when(place == p)
            def _():
                for kind in range(2):
                    col = slice((kind * per_z + i) * width, (kind * per_z + i + 1) * width)
                    for which, ref in enumerate((out, other)):
                        if ref is not None:
                            start = pl.multiple_of((share ^ which) * width, HD) if split > 1 else 0
                            ref[:rows, col] = parts[kind * n + p][:, pl.ds(start, width)]


def pack_kernel(split, per_z, n, scal, *refs):
    parts, outs = refs[: 2 * n], refs[2 * n :]
    pack_block(split, per_z, n, EARLY, scal, parts, outs[0])
    pack_block(split, per_z, n, 0, scal, parts, outs[1], outs[2] if split > 1 else None)


def dkv_kernel(hp, kvl, rows, js, halves, first_call, last_call, job, n_job, scal, *refs):
    n = len(js)
    own_ld = [j for j in js if j in (0, EARLY)]
    qg_refs, refs = refs[: n * halves], refs[n * halves :]
    ld_refs, refs = dict(zip(own_ld, refs)), refs[len(own_ld) :]
    k_ref, v_ref = refs[:2]
    priors, refs = ((None, refs[2:]) if first_call else (refs[2 : 2 + 2 * halves], refs[2 + 2 * halves :]))
    job_refs, refs = refs[:n_job], refs[n_job:]
    outs, refs = refs[: 2 if last_call else 2 * halves], refs[2 if last_call else 2 * halves :]
    pending = []
    if job is not None:
        job_out, job_scratch, job_sem = refs[0], refs[1], refs[2]
        refs = refs[3:]
        job(scal, *job_refs, job_scratch)
        copy = pltpu.make_async_copy(job_scratch, job_out, job_sem)
        copy.start()
        pending.append(copy)
    nh = kvl // halves
    sub = GROUP // hp
    for half in range(halves):
        first = ((scal[0] % 2) ^ half) * nh if halves > 1 else 0
        for g in range(nh):
            col = pl.ds(pl.multiple_of((scal[1] * kvl + first + g) * HD, HD), HD)
            here = slice(g * HD, (g + 1) * HD)
            k, v = k_ref[:, col], v_ref[:, col]
            dk = dv = None
            if priors:
                dk, dv = priors[2 * half][:, here], priors[2 * half + 1][:, here]
            for at, j in enumerate(js):
                qg = qg_refs[half * n + at]
                base = g * GROUP * HD
                qs = stack_heads(qg, rows, base, GROUP)
                gs = stack_heads(qg, rows, nh * GROUP * HD + base, GROUP)
                units = []
                for u in range(sub):
                    unit = (first + g) * sub + u
                    if j in own_ld:
                        units.append(ld_refs[j][unit])
                    else:
                        thirds = [qg[rows:, t * rows : (t + 1) * rows].astype(F32) for t in range(3)]
                        flat = thirds[0] + thirds[1] + thirds[2]
                        total = flat[: 2 * hp]
                        for m in range(1, kvl * sub):
                            total = jnp.where(unit == m, flat[m * 2 * hp : (m + 1) * 2 * hp], total)
                        units.append(total)
                norm = jnp.concatenate(
                    [units[h // hp][h % hp : h % hp + 1] for h in range(GROUP)], axis=1
                )
                delta = jnp.concatenate(
                    [units[h // hp][hp + h % hp : hp + h % hp + 1] for h in range(GROUP)], axis=1
                )
                s = dot(k, qs, NT)
                e = jnp.exp2(s * SCALE2 - norm)
                gp = dot(v, gs, NT)
                ds = (e * (gp - delta)).astype(BF16)
                dv_z = dot(e.astype(BF16), gs, NN)
                dk_z = dot(ds, qs, NN)
                dv = dv_z if dv is None else dv + dv_z
                dk = dk_z if dk is None else dk + dk_z
            if last_call:
                done, sem = refs[0], refs[1]
                mine = pl.ds(pl.multiple_of((first + g) * HD, HD), HD)
                for kind, x in enumerate((dk * FACTOR, dv)):
                    buf = done.at[half * nh + g, kind]
                    buf[...] = x.astype(BF16)
                    copy = pltpu.make_async_copy(buf, outs[kind].at[:, mine], sem.at[half * nh + g, kind])
                    copy.start()
                    pending.append(copy)
            else:
                outs[2 * half][:, here] = dk
                outs[2 * half + 1][:, here] = dv
    for copy in pending:
        copy.wait()


def dkv_call(js, qg, rows, keys, values, ld, hp, kvl, priors=(), last=False, job=None):
    halves = len(qg)
    nk = keys.shape[0]
    out = [shaped((nk, kvl * HD), BF16)] * 2
    if not last:
        out = [shaped((nk, kvl // halves * HD), F32)] * (2 * halves)
    scratch, hbm, job_args, n_out = [], (0, 1) if last else (), [], len(out)
    kernel = None
    if job is not None:
        kernel, job_args, job_shape = job
        out = out + [job_shape]
        hbm += (n_out,)
        scratch += [pltpu.VMEM(job_shape.shape, job_shape.dtype), pltpu.SemaphoreType.DMA(())]
    if last:
        scratch += [pltpu.VMEM((kvl, 2, nk, HD), BF16), pltpu.SemaphoreType.DMA((kvl, 2))]
    args = [half[j] for half in qg for j in js] + [ld[j] for j in js if j in (0, EARLY)]
    return call(
        functools.partial(
            dkv_kernel, hp, kvl, rows, js, halves, not priors, last, kernel, len(job_args)
        ),
        out,
        args + [keys, values] + list(priors) + job_args,
        flops=8 * len(js) * rows * GROUP * kvl * nk * HD,
        limit=24 * MIB,
        hbm=hbm,
        scratch=scratch,
    )


def sum_kernel(scal, *refs):
    total = refs[0][...].astype(F32)
    for r in refs[1:-1]:
        total += r[...].astype(F32)
    refs[-1][...] = total.astype(BF16)


def program(queries, keys, values, out_grad):
    n_key, n_qry = lax.axis_size("key"), lax.axis_size("qry")
    rows, wide = queries.shape
    hps = HQ // n_key
    hp = min(hps, GROUP)
    ups = hps // hp
    kvl = KVH // n_qry
    per_z = n_key // n_qry
    split = 2 if (kvl % 2 == 0 and per_z == 1) else 1
    unit_z = kvl * GROUP // hp

    def swap(x, p, axis="key"):
        if p == 0:
            return x
        return lax.ppermute(x, axis, [(i, i ^ p) for i in range(lax.axis_size(axis))])

    q, g = {0: queries}, {0: out_grad}
    bit = n_key // 2
    while bit:
        for p in list(q):
            q[p ^ bit] = swap(q[p], bit)
            g[p ^ bit] = swap(g[p], bit)
        bit //= 2

    o_part, e_part, st = {}, {}, {}
    for p in range(0, n_key, 2):
        after = [] if p else [warm_call()]
        o, e, st[p] = fwd_call((p, p + 1), q, keys, values, hp, ups, after)
        for at in range(2):
            o_part[p + at], e_part[p + at] = o[at], e[at]
    ql, gl, ol = ([x[p] for p in range(n_key)] for x in (q, g, o_part))

    width = 2 * per_z * wide // split
    block = shaped((rows, width), BF16)
    early, *own_blocks = call(
        functools.partial(pack_kernel, split, per_z, n_key), [block] * (1 + split), ql + gl
    )

    def delta_call(places, stats, whole=0):
        n = whole or len(places) * ups
        return call(
            functools.partial(delta_kernel, hp, ups, places, whole),
            shaped((n, 3 * hp, rows), F32),
            [ol[p] for p in places] + [gl[p] for p in places] + stats,
        )

    own = delta_call((0, 1), [st[0]])
    remote = [st[p] for p in range(2, n_key, 2)]
    own = delta_call(tuple(range(2, n_key)), remote + [own], n_key * ups)
    stats = [swap(own, p) for p in range(n_key)]
    o_recv = [swap(ol[p], p) for p in range(n_key)]
    late = tuple(j for j in range(1, n_qry) if j != EARLY)
    units = shaped((unit_z, 2 * hp, rows), F32)
    ld, ld_own, ld_early, *late_blocks = call(
        functools.partial(stats_kernel, hp, ups, n_key, unit_z, late, split, per_z),
        [shaped((n_key * ups, 2 * hp, rows), F32), units, units]
        + [shaped((rows + unit_z * 2 * hp, width), BF16)] * len(late),
        stats + ql + gl,
    )
    mine_z = {0: own_blocks[0], EARLY: swap(early, EARLY, "qry")}
    for j, x in zip(late, late_blocks):
        mine_z[j] = swap(x, j, "qry")
    ld_z = {0: ld_own, EARLY: swap(ld_early, EARLY, "qry")}

    dq_recv = [None] * n_key
    for p in reversed(range(0, n_key, 2)):
        dqs = dq_call((p, p + 1), e_part, g, keys, values, ld, own, hp, ups)
        for at, dq in enumerate(dqs):
            dq_recv[p + at] = swap(dq, p + at)

    blocks = [mine_z]
    if split == 2:
        blocks.append({0: own_blocks[1]})
        for j in range(1, n_qry):
            blocks[1][j] = swap(mine_z[j], 1)
    result = shaped((rows, wide), BF16)
    combine = (functools.partial(out_kernel, hp, ups, n_key), [ld] + stats + o_recv, result)
    total = (sum_kernel, dq_recv, result)

    def add(js, priors=(), last=False, job=None):
        return dkv_call(js, blocks, rows, keys, values, ld_z, hp, kvl, priors, last, job)

    acc = add((0,))
    *acc, attn_out = add((EARLY,), acc, job=combine)
    key_out, value_out, query_out = add(late, acc, last=True, job=total)
    return (attn_out, query_out, key_out, value_out)


def solution(mesh):
    in_specs = (
        P(("ckpt", "qry"), "key"),
        P(("ckpt", "key"), None),
        P(("ckpt", "key"), None),
        P(("ckpt", "qry"), "key"),
    )
    out_specs = (
        P(("ckpt", "qry"), "key"),
        P(("ckpt", "qry"), "key"),
        P(("ckpt", "key"), "qry"),
        P(("ckpt", "key"), "qry"),
    )
    return jax.shard_map(
        program, mesh=mesh, in_specs=in_specs, out_specs=out_specs, check_vma=False
    )
```
